32 devices in a mesh: group: 2 (over y), dev: 16 (over z, x, core).
Axes of the slice: x: 2, y: 2, z: 4, core: 2. Of those that a mesh axis runs over, the one named last changes fastest.
Arguments:
- bin_index: int32 [131072, 128], P(('group', 'dev')), may hold values from 0 to 63
- gradient: bfloat16 [131072], P(('group', 'dev')), may hold values from -6 to 6
- hessian: bfloat16 [131072], P(('group', 'dev')), may hold values from 0.049804688 to 0.25
- child_id: int32 [131072], P(('group', 'dev')), may hold values from 0 to 63
- smaller_side: int32 [32], replicated, may hold values from 0 to 1
Outputs:
- best_gain: float32 [32, 128], P('group', 'dev')
- child_best: float32 [32], P('group')
The draws below stay inside these ranges and needn't reach their ends.
All inputs are finite; a program needn't handle non-finite values.
Results may differ from the reference program's by a relative error of at most 0.0003.
Values sent between devices are 32-bit elements; how exact they have to be, the bound alone decides.
A program may use at most 64 MiB of HBM per device.

```python
import math
import jax
import jax.numpy as jnp
from jax import lax

FEAT = 128
BINS = 64
PAIRS = 32
ROWS = 131072


def place_ends(values, own_key, least, largest):
    spot = [jax.random.randint(jax.random.fold_in(own_key, axis), (), 0, length) for axis, length in enumerate(values.shape)]
    main_axis = values.shape.index(max(values.shape))
    beside = spot[:main_axis] + [(spot[main_axis] + 1) % values.shape[main_axis]] + spot[main_axis + 1:]
    return values.at[tuple(spot)].set(least).at[tuple(beside)].set(largest)


def shard_levels(own_key, extent, cuts, low, top_value):
    loudness = 1.0
    for position, parts in cuts:
        draws = jax.random.uniform(jax.random.fold_in(jax.random.fold_in(own_key, 6), position), (parts,), jnp.float32, low / len(cuts), top_value / len(cuts))
        loudness = loudness * jnp.repeat(jnp.exp(draws), extent[position] // parts).reshape((-1,) + (1,) * (len(extent) - 1 - position))
    return loudness


def gaussian(own_key, extent, deviation, reach, cuts=(), kind=jnp.bfloat16):
    result = deviation * jax.random.normal(own_key, extent, jnp.float32)
    if cuts:
        result = result * shard_levels(own_key, extent, cuts, -0.22, 0.18)
    return jnp.clip(result, -reach, reach).astype(kind)


def setup_inputs(seed: int = 0) -> dict:
    key_list = jax.random.split(jax.random.key(seed), 6)
    return {
        "bin_index": place_ends(jax.random.randint(key_list[0], (ROWS, FEAT), 0, BINS), jax.random.fold_in(key_list[0], 1), 0, BINS - 1).astype(jnp.int32),
        "gradient": gaussian(key_list[1], (ROWS,), 1.0, 6.0, ((0, 32),)),
        "hessian": jnp.clip(0.049804688 + 0.20019531 * jax.random.uniform(key_list[2], (ROWS,), jnp.float32) ** shard_levels(key_list[2], (ROWS,), ((0, 32),), -0.2, 0.2), 0.049804688, 0.25).astype(jnp.bfloat16),
        "child_id": place_ends(jax.random.randint(key_list[3], (ROWS,), 0, 2 * PAIRS), jax.random.fold_in(key_list[3], 1), 0, (2 * PAIRS) - 1).astype(jnp.int32),
        "smaller_side": place_ends(jax.random.randint(key_list[4], (PAIRS,), 0, 2), jax.random.fold_in(key_list[4], 1), 0, 1).astype(jnp.int32),
    }


reg_lambda = 1.0


def split_gains(hist_grad, hist_hess):
    left_grad = jnp.cumsum(hist_grad, axis=-1)[..., :-1]
    left_hess = jnp.cumsum(hist_hess, axis=-1)[..., :-1]
    total_grad = jnp.sum(hist_grad, axis=-1, keepdims=True)
    total_hess = jnp.sum(hist_hess, axis=-1, keepdims=True)
    right_grad = total_grad - left_grad
    value = left_grad * left_grad / (left_hess + reg_lambda)
    value = value + right_grad * right_grad / (total_hess - left_hess + reg_lambda)
    value = value - total_grad * total_grad / (total_hess + reg_lambda)
    return jnp.max(value, axis=-1)


def reference(bin_index, gradient, hessian, child_id, smaller_side):
    row_count = bin_index.shape[0]
    pair_index = (child_id // 2).astype(jnp.int32)
    member = (child_id - 2 * pair_index == smaller_side[pair_index]).astype(jnp.float32)
    values = jnp.stack([gradient.astype(jnp.float32) * member, hessian.astype(jnp.float32) * member], axis=1)
    block_size = math.gcd(FEAT, 8)
    offsets = jnp.arange(block_size, dtype=jnp.int32) * (PAIRS * BINS)
    base_index = (pair_index * BINS).astype(jnp.int32)

    def one_block(number):
        columns = lax.dynamic_slice_in_dim(bin_index, (number * block_size).astype(jnp.int32), block_size, 1)
        segment = base_index[:, None] + columns + offsets[None, :]
        spread = jnp.broadcast_to(values[:, None, :], (row_count, block_size, 2))
        summed = jax.ops.segment_sum(spread.reshape(-1, 2), segment.reshape(-1).astype(jnp.int32), num_segments=block_size * PAIRS * BINS)
        return summed.reshape(block_size, PAIRS, BINS, 2)

    hist = lax.map(one_block, jnp.arange(FEAT // block_size, dtype=jnp.int32)).reshape(FEAT, PAIRS, BINS, 2)
    best_gain = split_gains(hist[..., 0], hist[..., 1]).T
    child_best = jnp.max(best_gain, axis=1)
    return best_gain, child_best
```

```python
import functools

import jax
import jax.numpy as jnp
from jax import lax
from jax.experimental import pallas as pl
from jax.experimental.pallas import tpu as pltpu
from jax.sharding import PartitionSpec as P

BINS = 64
LANES = 128
KCHUNK = 1024


reg_lambda = 1.0


def split_gains(hist_grad, hist_hess):
    left_grad = jnp.cumsum(hist_grad, axis=-1)[..., :-1]
    left_hess = jnp.cumsum(hist_hess, axis=-1)[..., :-1]
    total_grad = jnp.sum(hist_grad, axis=-1, keepdims=True)
    total_hess = jnp.sum(hist_hess, axis=-1, keepdims=True)
    right_grad = total_grad - left_grad
    value = left_grad * left_grad / (left_hess + reg_lambda)
    value = value + right_grad * right_grad / (total_hess - left_hess + reg_lambda)
    value = value - total_grad * total_grad / (total_hess + reg_lambda)
    return jnp.max(value, axis=-1)


def plain_body(bin_index, gradient, hessian, child_id, smaller_side):
    leaves = smaller_side.shape[0]
    features = bin_index.shape[1]
    target = 2 * jnp.arange(leaves, dtype=jnp.int32)[None, :] + smaller_side[None, :]
    chosen = child_id[:, None] == target
    nothing = jnp.zeros((), jnp.bfloat16)
    weights = jnp.concatenate(
        [
            jnp.where(chosen, gradient[:, None], nothing),
            jnp.where(chosen, hessian[:, None], nothing),
        ],
        axis=1,
    )
    levels = jnp.arange(BINS, dtype=jnp.int32)

    def one_feature(column):
        onehot = (column[:, None] == levels[None, :]).astype(jnp.bfloat16)
        product = lax.dot_general(
            weights, onehot, (((0,), (0,)), ((), ())), preferred_element_type=jnp.float32
        )
        return product.reshape(2, leaves, BINS).transpose(1, 0, 2).reshape(leaves, 2 * BINS)

    stacked = lax.map(one_feature, bin_index.T)
    owned = lax.psum_scatter(stacked, "dev", scatter_dimension=0, tiled=True)
    owned = lax.psum_scatter(owned, "group", scatter_dimension=1, tiled=True)
    hist_grad = owned[:, :, :BINS].transpose(1, 0, 2)
    hist_hess = owned[:, :, BINS:].transpose(1, 0, 2)
    best_gain = split_gains(hist_grad, hist_hess)
    child_best = lax.pmax(jnp.max(best_gain, axis=1), "dev")
    return (best_gain, child_best)


def kernel(
    groups, devs, leaves,
    bins_ref, grad_ref, hess_ref, child_ref, side_ref,
    gain_ref, best_ref,
    bins_t, weights, pair_out, pair_in, mine_out, mine_in, best_out, best_in,
    pair_send, pair_recv, mine_send, mine_recv, best_send, best_recv,
):
    rows, features = bins_ref.shape
    own_features = features // devs
    own_leaves = leaves // groups
    width = 2 * own_leaves
    slots = LANES // width
    quads = own_features // slots
    chips = devs // 2
    me_g = lax.axis_index("group")
    me_d = lax.axis_index("dev")
    me_c = lax.rem(me_d, 2)
    me_j = lax.div(me_d, 2)
    barrier = pltpu.get_barrier_semaphore()

    def at(g, d):
        return {"group": g, "dev": d}

    greeted = 0
    for step in range(1, devs):
        other = lax.rem(me_d + step, devs)
        pl.semaphore_signal(barrier, inc=1, device_id=at(me_g, other), device_id_type=pl.DeviceIdType.MESH)
        greeted += 1
    for turn in range(1, groups):
        for step in range(chips):
            other = lax.rem(me_j + step, chips) * 2 + me_c
            pl.semaphore_signal(
                barrier, inc=1, device_id=at(lax.rem(me_g + turn, groups), other),
                device_id_type=pl.DeviceIdType.MESH,
            )
            greeted += 1

    columns = groups * LANES
    column = lax.broadcasted_iota(jnp.int32, (columns, 1), 0)
    within = lax.rem(column, width)
    leaf = lax.div(column, LANES) * own_leaves + lax.rem(within, own_leaves)
    target = jnp.zeros_like(leaf)
    for number in range(leaves):
        target = jnp.where(leaf == number, 2 * number + side_ref[number], target)
    is_grad = within < own_leaves
    step_rows = min(rows, 512)

    def prepare(number, carry):
        here = pl.ds(pl.multiple_of(number * step_rows, step_rows), step_rows)
        child = child_ref[:, here]
        grad = grad_ref[:, here].astype(jnp.float32)
        hess = hess_ref[:, here].astype(jnp.float32)
        value = jnp.where(is_grad, grad, hess)
        value = jnp.where(child == target, value, 0.0)
        weights[here, :] = value.T.astype(jnp.bfloat16)
        bins_t[:, here] = bins_ref[here, :].astype(jnp.float32).T
        return carry

    lax.fori_loop(0, rows // step_rows, prepare, 0)
    pl.semaphore_wait(barrier, greeted)

    chunk = min(rows, KCHUNK)
    pack = 16
    level = lax.broadcasted_iota(jnp.int32, (pack, chunk), 0).astype(jnp.float32).astype(jnp.bfloat16)
    one = jnp.ones((), jnp.bfloat16)
    zero = jnp.zeros((), jnp.bfloat16)
    lane = lax.broadcasted_iota(jnp.int32, (BINS, LANES), 1)

    def block(d):
        base = pl.multiple_of(d * own_features, own_features)
        total = None
        for start in range(0, rows, chunk):
            parts = []
            values = bins_t[pl.ds(base, own_features), start:start + chunk]
            for f in range(own_features):
                row = jnp.broadcast_to(values[f:f + 1, :], (pack, chunk)).astype(jnp.bfloat16)
                for low in range(0, BINS, pack):
                    parts.append(jnp.where(row == level + jnp.bfloat16(low), one, zero))
            onehot = jnp.concatenate(parts, axis=0)
            product = jnp.dot(onehot, weights[start:start + chunk, :], preferred_element_type=jnp.float32)
            total = product if total is None else total + product
        result = []
        for g in range(groups):
            for q in range(quads):
                piece = None
                for s in range(slots):
                    f = q * slots + s
                    here = total[f * BINS:(f + 1) * BINS, g * LANES:(g + 1) * LANES]
                    piece = here if piece is None else jnp.where(lane >= s * width, here, piece)
                result.append(piece)
        return result

    def pair_copy(j):
        return pltpu.make_async_remote_copy(
            src_ref=pair_out.at[j], dst_ref=pair_in.at[j],
            send_sem=pair_send.at[j], recv_sem=pair_recv.at[j],
            device_id=at(me_g, me_j * 2 + 1 - me_c), device_id_type=pl.DeviceIdType.MESH,
        )

    def mine_copy(j, turn):
        to_g = lax.rem(me_g + turn, groups)
        to_j = lax.rem(me_j + 1 + j, chips)
        return pltpu.make_async_remote_copy(
            src_ref=mine_out.at[j, to_g], dst_ref=mine_in.at[turn, j],
            send_sem=mine_send.at[turn, j], recv_sem=mine_recv.at[turn, j],
            device_id=at(to_g, to_j * 2 + me_c), device_id_type=pl.DeviceIdType.MESH,
        )

    def one_chip(j, carry):
        to_j = lax.rem(me_j + 1 + j, chips)
        pieces = block(to_j * 2 + 1 - me_c)
        for g in range(groups):
            for q in range(quads):
                pair_out[j, g, q * BINS:(q + 1) * BINS, :] = pieces[g * quads + q]
        pair_copy(j).start()
        pieces = block(to_j * 2 + me_c)
        pair_copy(j).wait()
        for g in range(groups):
            for q in range(quads):
                part = slice(q * BINS, (q + 1) * BINS)
                mine_out[j, g, part, :] = pieces[g * quads + q] + pair_in[j, g, part, :]
        for turn in range(1, groups):
            mine_copy(j, turn).start()

        @pl.when(j < chips - 1)
        def _():
            mine_copy(j, 0).start()

        return carry

    lax.fori_loop(0, chips, one_chip, 0)

    hist = mine_out[chips - 1, me_g]
    for turn in range(groups):
        for j in range(chips):
            if turn == 0 and j == chips - 1:
                continue
            mine_copy(j, turn).wait()
            hist = hist + mine_in[turn, j]

    bests = []
    for q in range(quads):
        left = hist[q * BINS:(q + 1) * BINS, :]
        shift = 1
        while shift < BINS:
            left = left + jnp.concatenate(
                [jnp.zeros((shift, LANES), jnp.float32), left[:BINS - shift, :]], axis=0
            )
            shift *= 2
        both = pltpu.roll(left, LANES - own_leaves, 1)
        left_grad, left_hess = left, both
        total_grad, total_hess = left[BINS - 1:, :], both[BINS - 1:, :]
        right_grad = total_grad - left_grad
        usable = lax.rem(lane, width) < own_leaves
        left_hess = jnp.where(usable, left_hess, 0.0)
        total_hess = jnp.where(usable[:1, :], total_hess, 0.0)
        value = left_grad * left_grad / (left_hess + reg_lambda)
        value = value + right_grad * right_grad / (total_hess - left_hess + reg_lambda)
        value = value - total_grad * total_grad / (total_hess + reg_lambda)
        row = lax.broadcasted_iota(jnp.int32, (BINS, LANES), 0)
        value = jnp.where(row < BINS - 1, value, -jnp.inf)
        bests.append(jnp.max(value, axis=0, keepdims=True))
    best = bests[0]
    for q in range(quads):
        gain_ref[q:q + 1, :] = bests[q]
        best = jnp.maximum(best, bests[q])
    best = jnp.broadcast_to(best, (8, LANES))
    move = width
    folded = best
    for s in range(1, slots):
        folded = jnp.maximum(folded, pltpu.roll(best, s * move, 1))
    best_out[...] = folded

    def best_copy(step):
        return pltpu.make_async_remote_copy(
            src_ref=best_out, dst_ref=best_in.at[step],
            send_sem=best_send.at[step], recv_sem=best_recv.at[step],
            device_id=at(me_g, lax.rem(me_d + step, devs)), device_id_type=pl.DeviceIdType.MESH,
        )

    for step in range(1, devs):
        best_copy(step).start()
    for step in range(1, devs):
        best_copy(step).wait()
        folded = jnp.maximum(folded, best_in[step])
    best_ref[...] = folded


def kernel_body(groups, devs, bin_index, gradient, hessian, child_id, smaller_side):
    rows, features = bin_index.shape
    leaves = smaller_side.shape[0]
    own_features = features // devs
    own_leaves = leaves // groups
    width = 2 * own_leaves
    slots = LANES // width
    quads = own_features // slots
    chips = devs // 2
    vmem = pl.BlockSpec(memory_space=pltpu.VMEM)
    gain, best = pl.pallas_call(
        functools.partial(kernel, groups, devs, leaves),
        out_shape=(
            jax.ShapeDtypeStruct((quads, LANES), jnp.float32),
            jax.ShapeDtypeStruct((8, LANES), jnp.float32),
        ),
        in_specs=[vmem, vmem, vmem, vmem, pl.BlockSpec(memory_space=pltpu.SMEM)],
        out_specs=(vmem, vmem),
        scratch_shapes=[
            pltpu.VMEM((features, rows), jnp.float32),
            pltpu.VMEM((rows, groups * LANES), jnp.bfloat16),
            pltpu.VMEM((chips, groups, quads * BINS, LANES), jnp.float32),
            pltpu.VMEM((chips, groups, quads * BINS, LANES), jnp.float32),
            pltpu.VMEM((chips, groups, quads * BINS, LANES), jnp.float32),
            pltpu.VMEM((groups, chips, quads * BINS, LANES), jnp.float32),
            pltpu.VMEM((8, LANES), jnp.float32),
            pltpu.VMEM((devs, 8, LANES), jnp.float32),
            pltpu.SemaphoreType.DMA((chips,)),
            pltpu.SemaphoreType.DMA((chips,)),
            pltpu.SemaphoreType.DMA((groups, chips)),
            pltpu.SemaphoreType.DMA((groups, chips)),
            pltpu.SemaphoreType.DMA((devs,)),
            pltpu.SemaphoreType.DMA((devs,)),
        ],
        compiler_params=pltpu.CompilerParams(
            collective_id=0, has_side_effects=True, vmem_limit_bytes=48 * 1024 * 1024
        ),
    )(
        bin_index, gradient.reshape(1, rows), hessian.reshape(1, rows),
        child_id.reshape(1, rows), smaller_side,
    )
    best_gain = gain.reshape(quads, slots, width)[:, :, :own_leaves]
    best_gain = best_gain.transpose(2, 0, 1).reshape(own_leaves, own_features)
    return (best_gain, best[0, :own_leaves])


def fits(groups, devs, leaves, features, rows):
    if devs % 2 or features % devs or leaves % groups:
        return False
    width = 2 * (leaves // groups)
    if LANES % width:
        return False
    slots = LANES // width
    own = features // devs
    return own % slots == 0 and own % 8 == 0 and rows % KCHUNK == 0 and devs <= 16


def solution(mesh):
    in_specs = (
        P(("group", "dev"), None),
        P(("group", "dev")),
        P(("group", "dev")),
        P(("group", "dev")),
        P(),
    )
    out_specs = (P("group", "dev"), P("group"))
    groups, devs = mesh.shape["group"], mesh.shape["dev"]

    def body(bin_index, gradient, hessian, child_id, smaller_side):
        rows, features = bin_index.shape
        args = (bin_index, gradient, hessian, child_id, smaller_side)
        if fits(groups, devs, smaller_side.shape[0], features, rows):
            return kernel_body(groups, devs, *args)
        return plain_body(*args)

    return jax.shard_map(body, mesh=mesh, in_specs=in_specs, out_specs=out_specs, check_vma=False)
```

```python
import functools

import jax
import jax.numpy as jnp
from jax import lax
from jax.experimental import pallas as pl
from jax.experimental.pallas import tpu as pltpu
from jax.sharding import PartitionSpec as P

BINS = 64
LANES = 128
KCHUNK = 1024


reg_lambda = 1.0


def split_gains(hist_grad, hist_hess):
    left_grad = jnp.cumsum(hist_grad, axis=-1)[..., :-1]
    left_hess = jnp.cumsum(hist_hess, axis=-1)[..., :-1]
    total_grad = jnp.sum(hist_grad, axis=-1, keepdims=True)
    total_hess = jnp.sum(hist_hess, axis=-1, keepdims=True)
    right_grad = total_grad - left_grad
    value = left_grad * left_grad / (left_hess + reg_lambda)
    value = value + right_grad * right_grad / (total_hess - left_hess + reg_lambda)
    value = value - total_grad * total_grad / (total_hess + reg_lambda)
    return jnp.max(value, axis=-1)


def plain_body(bin_index, gradient, hessian, child_id, smaller_side):
    leaves = smaller_side.shape[0]
    features = bin_index.shape[1]
    target = 2 * jnp.arange(leaves, dtype=jnp.int32)[None, :] + smaller_side[None, :]
    chosen = child_id[:, None] == target
    nothing = jnp.zeros((), jnp.bfloat16)
    weights = jnp.concatenate(
        [
            jnp.where(chosen, gradient[:, None], nothing),
            jnp.where(chosen, hessian[:, None], nothing),
        ],
        axis=1,
    )
    levels = jnp.arange(BINS, dtype=jnp.int32)

    def one_feature(column):
        onehot = (column[:, None] == levels[None, :]).astype(jnp.bfloat16)
        product = lax.dot_general(
            weights, onehot, (((0,), (0,)), ((), ())), preferred_element_type=jnp.float32
        )
        return product.reshape(2, leaves, BINS).transpose(1, 0, 2).reshape(leaves, 2 * BINS)

    stacked = lax.map(one_feature, bin_index.T)
    owned = lax.psum_scatter(stacked, "dev", scatter_dimension=0, tiled=True)
    owned = lax.psum_scatter(owned, "group", scatter_dimension=1, tiled=True)
    hist_grad = owned[:, :, :BINS].transpose(1, 0, 2)
    hist_hess = owned[:, :, BINS:].transpose(1, 0, 2)
    best_gain = split_gains(hist_grad, hist_hess)
    child_best = lax.pmax(jnp.max(best_gain, axis=1), "dev")
    return (best_gain, child_best)


def kernel(
    groups, devs, leaves,
    bins_ref, grad_ref, hess_ref, child_ref, side_ref,
    gain_ref, best_ref,
    bins_t, weights, pair_out, pair_in, side_out, side_in, mine, far_in, near_in, best_out, best_in,
    pair_send, pair_recv, side_send, side_recv, far_send, far_recv, near_send, near_recv,
    best_send, best_recv,
):
    rows, features = bins_ref.shape
    own_features = features // devs
    own_leaves = leaves // groups
    width = 2 * own_leaves
    slots = LANES // width
    quads = own_features // slots
    chips = devs // 2
    me_g = lax.axis_index("group")
    me_d = lax.axis_index("dev")
    me_c = lax.rem(me_d, 2)
    me_j = lax.div(me_d, 2)
    planes = chips // 2
    me_x = lax.rem(me_j, 2)
    me_z = lax.div(me_j, 2)
    barrier = pltpu.get_barrier_semaphore()

    def at(g, d):
        return {"group": g, "dev": d}

    greeted = 0
    for step in range(1, devs):
        other = lax.rem(me_d + step, devs)
        pl.semaphore_signal(barrier, inc=1, device_id=at(me_g, other), device_id_type=pl.DeviceIdType.MESH)
        greeted += 1
    for turn in range(1, groups):
        for step in range(chips):
            other = lax.rem(me_j + step, chips) * 2 + me_c
            pl.semaphore_signal(
                barrier, inc=1, device_id=at(lax.rem(me_g + turn, groups), other),
                device_id_type=pl.DeviceIdType.MESH,
            )
            greeted += 1

    columns = groups * LANES
    column = lax.broadcasted_iota(jnp.int32, (columns, 1), 0)
    within = lax.rem(column, width)
    leaf = lax.div(column, LANES) * own_leaves + lax.rem(within, own_leaves)
    target = jnp.zeros_like(leaf)
    for number in range(leaves):
        target = jnp.where(leaf == number, 2 * number + side_ref[number], target)
    is_grad = within < own_leaves
    step_rows = min(rows, 512)

    def prepare(number, carry):
        here = pl.ds(pl.multiple_of(number * step_rows, step_rows), step_rows)
        child = child_ref[:, here]
        grad = grad_ref[:, here].astype(jnp.float32)
        hess = hess_ref[:, here].astype(jnp.float32)
        value = jnp.where(is_grad, grad, hess)
        value = jnp.where(child == target, value, 0.0)
        weights[here, :] = value.T.astype(jnp.bfloat16)
        bins_t[:, here] = bins_ref[here, :].astype(jnp.float32).T
        return carry

    lax.fori_loop(0, rows // step_rows, prepare, 0)
    pl.semaphore_wait(barrier, greeted)

    chunk = min(rows, KCHUNK)
    pack = 16
    level = lax.broadcasted_iota(jnp.int32, (pack, chunk), 0).astype(jnp.float32).astype(jnp.bfloat16)
    one = jnp.ones((), jnp.bfloat16)
    zero = jnp.zeros((), jnp.bfloat16)
    lane = lax.broadcasted_iota(jnp.int32, (BINS, LANES), 1)

    def block(d):
        base = pl.multiple_of(d * own_features, own_features)
        total = None
        for start in range(0, rows, chunk):
            parts = []
            values = bins_t[pl.ds(base, own_features), start:start + chunk]
            for f in range(own_features):
                row = jnp.broadcast_to(values[f:f + 1, :], (pack, chunk)).astype(jnp.bfloat16)
                for low in range(0, BINS, pack):
                    parts.append(jnp.where(row == level + jnp.bfloat16(low), one, zero))
            onehot = jnp.concatenate(parts, axis=0)
            product = jnp.dot(onehot, weights[start:start + chunk, :], preferred_element_type=jnp.float32)
            total = product if total is None else total + product
        result = []
        for g in range(groups):
            for q in range(quads):
                piece = None
                for s in range(slots):
                    f = q * slots + s
                    here = total[f * BINS:(f + 1) * BINS, g * LANES:(g + 1) * LANES]
                    piece = here if piece is None else jnp.where(lane >= s * width, here, piece)
                result.append(piece)
        return result

    def pair_copy(j):
        return pltpu.make_async_remote_copy(
            src_ref=pair_out.at[j], dst_ref=pair_in.at[j],
            send_sem=pair_send.at[j], recv_sem=pair_recv.at[j],
            device_id=at(me_g, me_j * 2 + 1 - me_c), device_id_type=pl.DeviceIdType.MESH,
        )

    def side_copy(k):
        return pltpu.make_async_remote_copy(
            src_ref=side_out.at[k], dst_ref=side_in.at[k],
            send_sem=side_send.at[k], recv_sem=side_recv.at[k],
            device_id=at(me_g, (me_z * 2 + 1 - me_x) * 2 + me_c), device_id_type=pl.DeviceIdType.MESH,
        )

    def far_copy(k, turn):
        to_g = lax.rem(me_g + turn, groups)
        return pltpu.make_async_remote_copy(
            src_ref=mine.at[k, to_g], dst_ref=far_in.at[turn, k],
            send_sem=far_send.at[turn, k], recv_sem=far_recv.at[turn, k],
            device_id=at(to_g, (lax.rem(me_z + 1 + k, planes) * 2 + me_x) * 2 + me_c),
            device_id_type=pl.DeviceIdType.MESH,
        )

    def near_copy(turn):
        to_g = lax.rem(me_g + turn, groups)
        return pltpu.make_async_remote_copy(
            src_ref=side_out.at[planes - 1, to_g], dst_ref=near_in.at[turn],
            send_sem=near_send.at[turn], recv_sem=near_recv.at[turn],
            device_id=at(to_g, (me_z * 2 + 1 - me_x) * 2 + me_c), device_id_type=pl.DeviceIdType.MESH,
        )

    def owner(j):
        to_z = lax.rem(me_z + 1 + lax.div(j, 2), planes)
        to_x = lax.rem(me_x + 1 + lax.rem(j, 2), 2)
        return (to_z * 2 + to_x) * 2

    def send_pair(j):
        pieces = block(owner(j) + 1 - me_c)
        for g in range(groups):
            for q in range(quads):
                pair_out[j, g, q * BINS:(q + 1) * BINS, :] = pieces[g * quads + q]
        pair_copy(j).start()

    send_pair(0)

    def one_step(j, carry):
        k = lax.div(j, 2)
        odd = lax.rem(j, 2)

        @pl.when(j < chips - 1)
        def _():
            send_pair(j + 1)

        pieces = block(owner(j) + me_c)
        pair_copy(j).wait()

        def put(ref):
            for g in range(groups):
                for q in range(quads):
                    part = slice(q * BINS, (q + 1) * BINS)
                    ref[k, g, part, :] = pieces[g * quads + q] + pair_in[j, g, part, :]

        @pl.when(odd == 0)
        def _():
            put(side_out)

            @pl.when(k < planes - 1)
            def _():
                side_copy(k).start()

            @pl.when(k == planes - 1)
            def _():
                for turn in range(groups):
                    near_copy(turn).start()

            @pl.when(k > 0)
            def _():
                side_copy(k - 1).wait()
                for g in range(groups):
                    mine[k - 1, g] = mine[k - 1, g] + side_in[k - 1, g]
                for turn in range(groups):
                    far_copy(k - 1, turn).start()

        @pl.when(odd == 1)
        def _():
            put(mine)

            @pl.when(k == planes - 1)
            def _():
                for turn in range(1, groups):
                    far_copy(planes - 1, turn).start()

        return carry

    lax.fori_loop(0, chips, one_step, 0)

    hist = mine[planes - 1, me_g]
    for k in range(planes - 1):
        for turn in range(groups):
            far_copy(k, turn).wait()
            hist = hist + far_in[turn, k]
    for turn in range(groups):
        near_copy(turn).wait()
        hist = hist + near_in[turn]
    for turn in range(1, groups):
        far_copy(planes - 1, turn).wait()
        hist = hist + far_in[turn, planes - 1]

    bests = []
    for q in range(quads):
        left = hist[q * BINS:(q + 1) * BINS, :]
        shift = 1
        while shift < BINS:
            left = left + jnp.concatenate(
                [jnp.zeros((shift, LANES), jnp.float32), left[:BINS - shift, :]], axis=0
            )
            shift *= 2
        both = pltpu.roll(left, LANES - own_leaves, 1)
        left_grad, left_hess = left, both
        total_grad, total_hess = left[BINS - 1:, :], both[BINS - 1:, :]
        right_grad = total_grad - left_grad
        usable = lax.rem(lane, width) < own_leaves
        left_hess = jnp.where(usable, left_hess, 0.0)
        total_hess = jnp.where(usable[:1, :], total_hess, 0.0)
        value = left_grad * left_grad / (left_hess + reg_lambda)
        value = value + right_grad * right_grad / (total_hess - left_hess + reg_lambda)
        value = value - total_grad * total_grad / (total_hess + reg_lambda)
        row = lax.broadcasted_iota(jnp.int32, (BINS, LANES), 0)
        value = jnp.where(row < BINS - 1, value, -jnp.inf)
        bests.append(jnp.max(value, axis=0, keepdims=True))
    best = bests[0]
    for q in range(quads):
        gain_ref[q:q + 1, :] = bests[q]
        best = jnp.maximum(best, bests[q])
    best = jnp.broadcast_to(best, (8, LANES))
    move = width
    folded = best
    for s in range(1, slots):
        folded = jnp.maximum(folded, pltpu.roll(best, s * move, 1))
    best_out[...] = folded

    def best_copy(step):
        return pltpu.make_async_remote_copy(
            src_ref=best_out, dst_ref=best_in.at[step],
            send_sem=best_send.at[step], recv_sem=best_recv.at[step],
            device_id=at(me_g, lax.rem(me_d + step, devs)), device_id_type=pl.DeviceIdType.MESH,
        )

    for step in range(1, devs):
        best_copy(step).start()
    for step in range(1, devs):
        best_copy(step).wait()
        folded = jnp.maximum(folded, best_in[step])
    best_ref[...] = folded


def kernel_body(groups, devs, bin_index, gradient, hessian, child_id, smaller_side):
    rows, features = bin_index.shape
    leaves = smaller_side.shape[0]
    own_features = features // devs
    own_leaves = leaves // groups
    width = 2 * own_leaves
    slots = LANES // width
    quads = own_features // slots
    chips = devs // 2
    planes = chips // 2
    vmem = pl.BlockSpec(memory_space=pltpu.VMEM)
    gain, best = pl.pallas_call(
        functools.partial(kernel, groups, devs, leaves),
        out_shape=(
            jax.ShapeDtypeStruct((quads, LANES), jnp.float32),
            jax.ShapeDtypeStruct((8, LANES), jnp.float32),
        ),
        in_specs=[vmem, vmem, vmem, vmem, pl.BlockSpec(memory_space=pltpu.SMEM)],
        out_specs=(vmem, vmem),
        scratch_shapes=[
            pltpu.VMEM((features, rows), jnp.float32),
            pltpu.VMEM((rows, groups * LANES), jnp.bfloat16),
            pltpu.VMEM((chips, groups, quads * BINS, LANES), jnp.float32),
            pltpu.VMEM((chips, groups, quads * BINS, LANES), jnp.float32),
            pltpu.VMEM((planes, groups, quads * BINS, LANES), jnp.float32),
            pltpu.VMEM((planes, groups, quads * BINS, LANES), jnp.float32),
            pltpu.VMEM((planes, groups, quads * BINS, LANES), jnp.float32),
            pltpu.VMEM((groups, planes, quads * BINS, LANES), jnp.float32),
            pltpu.VMEM((groups, quads * BINS, LANES), jnp.float32),
            pltpu.VMEM((8, LANES), jnp.float32),
            pltpu.VMEM((devs, 8, LANES), jnp.float32),
            pltpu.SemaphoreType.DMA((chips,)),
            pltpu.SemaphoreType.DMA((chips,)),
            pltpu.SemaphoreType.DMA((planes,)),
            pltpu.SemaphoreType.DMA((planes,)),
            pltpu.SemaphoreType.DMA((groups, planes)),
            pltpu.SemaphoreType.DMA((groups, planes)),
            pltpu.SemaphoreType.DMA((groups,)),
            pltpu.SemaphoreType.DMA((groups,)),
            pltpu.SemaphoreType.DMA((devs,)),
            pltpu.SemaphoreType.DMA((devs,)),
        ],
        compiler_params=pltpu.CompilerParams(
            collective_id=0, has_side_effects=True, vmem_limit_bytes=48 * 1024 * 1024
        ),
    )(
        bin_index, gradient.reshape(1, rows), hessian.reshape(1, rows),
        child_id.reshape(1, rows), smaller_side,
    )
    best_gain = gain.reshape(quads, slots, width)[:, :, :own_leaves]
    best_gain = best_gain.transpose(2, 0, 1).reshape(own_leaves, own_features)
    return (best_gain, best[0, :own_leaves])


def fits(groups, devs, leaves, features, rows):
    if devs % 4 or devs < 8 or features % devs or leaves % groups:
        return False
    width = 2 * (leaves // groups)
    if LANES % width:
        return False
    slots = LANES // width
    own = features // devs
    return own % slots == 0 and own % 8 == 0 and rows % KCHUNK == 0 and devs <= 16


def solution(mesh):
    in_specs = (
        P(("group", "dev"), None),
        P(("group", "dev")),
        P(("group", "dev")),
        P(("group", "dev")),
        P(),
    )
    out_specs = (P("group", "dev"), P("group"))
    groups, devs = mesh.shape["group"], mesh.shape["dev"]

    def body(bin_index, gradient, hessian, child_id, smaller_side):
        rows, features = bin_index.shape
        args = (bin_index, gradient, hessian, child_id, smaller_side)
        if fits(groups, devs, smaller_side.shape[0], features, rows):
            return kernel_body(groups, devs, *args)
        return plain_body(*args)

    return jax.shard_map(body, mesh=mesh, in_specs=in_specs, out_specs=out_specs, check_vma=False)
```

```python
import functools

import jax
import jax.numpy as jnp
from jax import lax
from jax.experimental import pallas as pl
from jax.experimental.pallas import tpu as pltpu
from jax.sharding import PartitionSpec as P

BINS = 64
LANES = 128
KCHUNK = 1024
STEP_ROWS = 512


reg_lambda = 1.0


def split_gains(hist_grad, hist_hess):
    left_grad = jnp.cumsum(hist_grad, axis=-1)[..., :-1]
    left_hess = jnp.cumsum(hist_hess, axis=-1)[..., :-1]
    total_grad = jnp.sum(hist_grad, axis=-1, keepdims=True)
    total_hess = jnp.sum(hist_hess, axis=-1, keepdims=True)
    right_grad = total_grad - left_grad
    value = left_grad * left_grad / (left_hess + reg_lambda)
    value = value + right_grad * right_grad / (total_hess - left_hess + reg_lambda)
    value = value - total_grad * total_grad / (total_hess + reg_lambda)
    return jnp.max(value, axis=-1)


def plain_body(bin_index, gradient, hessian, child_id, smaller_side):
    leaves = smaller_side.shape[0]
    features = bin_index.shape[1]
    target = 2 * jnp.arange(leaves, dtype=jnp.int32)[None, :] + smaller_side[None, :]
    chosen = child_id[:, None] == target
    nothing = jnp.zeros((), jnp.bfloat16)
    weights = jnp.concatenate(
        [
            jnp.where(chosen, gradient[:, None], nothing),
            jnp.where(chosen, hessian[:, None], nothing),
        ],
        axis=1,
    )
    levels = jnp.arange(BINS, dtype=jnp.int32)

    def one_feature(column):
        onehot = (column[:, None] == levels[None, :]).astype(jnp.bfloat16)
        product = lax.dot_general(
            weights, onehot, (((0,), (0,)), ((), ())), preferred_element_type=jnp.float32
        )
        return product.reshape(2, leaves, BINS).transpose(1, 0, 2).reshape(leaves, 2 * BINS)

    stacked = lax.map(one_feature, bin_index.T)
    owned = lax.psum_scatter(stacked, "dev", scatter_dimension=0, tiled=True)
    owned = lax.psum_scatter(owned, "group", scatter_dimension=1, tiled=True)
    hist_grad = owned[:, :, :BINS].transpose(1, 0, 2)
    hist_hess = owned[:, :, BINS:].transpose(1, 0, 2)
    best_gain = split_gains(hist_grad, hist_hess)
    child_best = lax.pmax(jnp.max(best_gain, axis=1), "dev")
    return (best_gain, child_best)


def kernel(
    groups, devs, leaves,
    bins_ref, grad_ref, hess_ref, child_ref, side_ref,
    gain_ref, best_ref,
    bins_v, grad_v, hess_v, child_v, values, bins_sem, small_sem,
    bins_t, weights, pair_out, pair_in, side_out, side_in, mine, far_in, near_in, best_out, best_in,
    pair_send, pair_recv, side_send, side_recv, far_send, far_recv, near_send, near_recv,
    best_send, best_recv,
):
    rows, features = bins_ref.shape
    own_features = features // devs
    own_leaves = leaves // groups
    width = 2 * own_leaves
    slots = LANES // width
    quads = own_features // slots
    chips = devs // 2
    me_g = lax.axis_index("group")
    me_d = lax.axis_index("dev")
    me_c = lax.rem(me_d, 2)
    me_j = lax.div(me_d, 2)
    planes = chips // 2
    me_x = lax.rem(me_j, 2)
    me_z = lax.div(me_j, 2)
    barrier = pltpu.get_barrier_semaphore()
    step_rows = STEP_ROWS

    def bins_copy(number):
        here = pl.ds(pl.multiple_of(number * step_rows, step_rows), step_rows)
        return pltpu.make_async_copy(bins_ref.at[here, :], bins_v.at[here, :], bins_sem.at[number])

    small = [
        pltpu.make_async_copy(source, place, small_sem.at[number])
        for number, (source, place) in enumerate(
            [(grad_ref, grad_v), (hess_ref, hess_v), (child_ref, child_v)]
        )
    ]
    for copy in small:
        copy.start()

    def at(g, d):
        return {"group": g, "dev": d}

    greeted = 0
    for step in range(1, devs):
        other = lax.rem(me_d + step, devs)
        pl.semaphore_signal(barrier, inc=1, device_id=at(me_g, other), device_id_type=pl.DeviceIdType.MESH)
        greeted += 1
    for turn in range(1, groups):
        for step in range(chips):
            other = lax.rem(me_j + step, chips) * 2 + me_c
            pl.semaphore_signal(
                barrier, inc=1, device_id=at(lax.rem(me_g + turn, groups), other),
                device_id_type=pl.DeviceIdType.MESH,
            )
            greeted += 1

    columns = groups * LANES
    column = lax.broadcasted_iota(jnp.int32, (columns, 1), 0)
    within = lax.rem(column, width)
    leaf = lax.div(column, LANES) * own_leaves + lax.rem(within, own_leaves)
    target = jnp.zeros_like(leaf)
    for number in range(leaves):
        target = jnp.where(leaf == number, 2 * number + side_ref[number], target)
    is_grad = within < own_leaves

    lax.fori_loop(0, rows // step_rows, lambda number, carry: (bins_copy(number).start(), carry)[1], 0)
    for copy in small:
        copy.wait()
    values[0] = grad_v[...].astype(jnp.float32)
    values[1] = hess_v[...].astype(jnp.float32)

    def prepare(number, carry):
        bins_copy(number).wait()
        here = pl.ds(pl.multiple_of(number * step_rows, step_rows), step_rows)
        bins_t[:, here] = bins_v[here, :].astype(jnp.float32).T
        for piece in range(step_rows // LANES):
            row = number * (step_rows // LANES) + piece
            value = jnp.where(is_grad, values[0, pl.ds(row, 1), :], values[1, pl.ds(row, 1), :])
            value = jnp.where(child_v[pl.ds(row, 1), :] == target, value, 0.0)
            there = pl.ds(pl.multiple_of(row * LANES, LANES), LANES)
            weights[there, :] = value.T.astype(jnp.bfloat16)
        return carry

    lax.fori_loop(0, rows // step_rows, prepare, 0)

    chunk = min(rows, KCHUNK)
    pack = 16
    level = lax.broadcasted_iota(jnp.int32, (pack, chunk), 0).astype(jnp.float32).astype(jnp.bfloat16)
    one = jnp.ones((), jnp.bfloat16)
    zero = jnp.zeros((), jnp.bfloat16)
    lane = lax.broadcasted_iota(jnp.int32, (BINS, LANES), 1)

    def block(d):
        base = pl.multiple_of(d * own_features, own_features)
        total = None
        for start in range(0, rows, chunk):
            parts = []
            levels = bins_t[pl.ds(base, own_features), start:start + chunk]
            for f in range(own_features):
                row = jnp.broadcast_to(levels[f:f + 1, :], (pack, chunk)).astype(jnp.bfloat16)
                for low in range(0, BINS, pack):
                    parts.append(jnp.where(row == level + jnp.bfloat16(low), one, zero))
            onehot = jnp.concatenate(parts, axis=0)
            product = jnp.dot(onehot, weights[start:start + chunk, :], preferred_element_type=jnp.float32)
            total = product if total is None else total + product
        result = []
        for g in range(groups):
            for q in range(quads):
                piece = None
                for s in range(slots):
                    f = q * slots + s
                    here = total[f * BINS:(f + 1) * BINS, g * LANES:(g + 1) * LANES]
                    piece = here if piece is None else jnp.where(lane >= s * width, here, piece)
                result.append(piece)
        return result

    def pair_copy(j):
        return pltpu.make_async_remote_copy(
            src_ref=pair_out.at[j], dst_ref=pair_in.at[j],
            send_sem=pair_send.at[j], recv_sem=pair_recv.at[j],
            device_id=at(me_g, me_j * 2 + 1 - me_c), device_id_type=pl.DeviceIdType.MESH,
        )

    def side_copy(k):
        return pltpu.make_async_remote_copy(
            src_ref=side_out.at[k], dst_ref=side_in.at[k],
            send_sem=side_send.at[k], recv_sem=side_recv.at[k],
            device_id=at(me_g, (me_z * 2 + 1 - me_x) * 2 + me_c), device_id_type=pl.DeviceIdType.MESH,
        )

    def far_copy(k, turn):
        to_g = lax.rem(me_g + turn, groups)
        return pltpu.make_async_remote_copy(
            src_ref=mine.at[k, to_g], dst_ref=far_in.at[turn, k],
            send_sem=far_send.at[turn, k], recv_sem=far_recv.at[turn, k],
            device_id=at(to_g, (lax.rem(me_z + 1 + k, planes) * 2 + me_x) * 2 + me_c),
            device_id_type=pl.DeviceIdType.MESH,
        )

    def near_copy(turn):
        to_g = lax.rem(me_g + turn, groups)
        return pltpu.make_async_remote_copy(
            src_ref=side_out.at[planes - 1, to_g], dst_ref=near_in.at[turn],
            send_sem=near_send.at[turn], recv_sem=near_recv.at[turn],
            device_id=at(to_g, (me_z * 2 + 1 - me_x) * 2 + me_c), device_id_type=pl.DeviceIdType.MESH,
        )

    def owner(j):
        to_z = lax.rem(me_z + 1 + lax.div(j, 2), planes)
        to_x = lax.rem(me_x + 1 + lax.rem(j, 2), 2)
        return (to_z * 2 + to_x) * 2

    def send_pair(j, first=False):
        pieces = block(owner(j) + 1 - me_c)
        if first:
            pl.semaphore_wait(barrier, greeted)
        for g in range(groups):
            for q in range(quads):
                pair_out[j, g, q * BINS:(q + 1) * BINS, :] = pieces[g * quads + q]
        pair_copy(j).start()

    send_pair(0, True)

    def one_step(j, carry):
        k = lax.div(j, 2)
        odd = lax.rem(j, 2)

        @pl.when(j < chips - 1)
        def _():
            send_pair(j + 1)

        pieces = block(owner(j) + me_c)
        pair_copy(j).wait()

        def put(ref):
            for g in range(groups):
                for q in range(quads):
                    part = slice(q * BINS, (q + 1) * BINS)
                    ref[k, g, part, :] = pieces[g * quads + q] + pair_in[j, g, part, :]

        @pl.when(odd == 0)
        def _():
            put(side_out)

            @pl.when(k < planes - 1)
            def _():
                side_copy(k).start()

            @pl.when(k == planes - 1)
            def _():
                for turn in range(groups):
                    near_copy(turn).start()

            @pl.when(k > 0)
            def _():
                side_copy(k - 1).wait()
                for g in range(groups):
                    mine[k - 1, g] = mine[k - 1, g] + side_in[k - 1, g]
                for turn in range(groups):
                    far_copy(k - 1, turn).start()

        @pl.when(odd == 1)
        def _():
            put(mine)

            @pl.when(k == planes - 1)
            def _():
                for turn in range(1, groups):
                    far_copy(planes - 1, turn).start()

        return carry

    lax.fori_loop(0, chips, one_step, 0)

    hist = mine[planes - 1, me_g]
    for k in range(planes - 1):
        for turn in range(groups):
            far_copy(k, turn).wait()
            hist = hist + far_in[turn, k]
    for turn in range(groups):
        near_copy(turn).wait()
        hist = hist + near_in[turn]
    for turn in range(1, groups):
        far_copy(planes - 1, turn).wait()
        hist = hist + far_in[turn, planes - 1]

    bests = []
    for q in range(quads):
        left = hist[q * BINS:(q + 1) * BINS, :]
        shift = 1
        while shift < BINS:
            left = left + jnp.concatenate(
                [jnp.zeros((shift, LANES), jnp.float32), left[:BINS - shift, :]], axis=0
            )
            shift *= 2
        both = pltpu.roll(left, LANES - own_leaves, 1)
        left_grad, left_hess = left, both
        total_grad, total_hess = left[BINS - 1:, :], both[BINS - 1:, :]
        right_grad = total_grad - left_grad
        usable = lax.rem(lane, width) < own_leaves
        left_hess = jnp.where(usable, left_hess, 0.0)
        total_hess = jnp.where(usable[:1, :], total_hess, 0.0)
        value = left_grad * left_grad / (left_hess + reg_lambda)
        value = value + right_grad * right_grad / (total_hess - left_hess + reg_lambda)
        value = value - total_grad * total_grad / (total_hess + reg_lambda)
        row = lax.broadcasted_iota(jnp.int32, (BINS, LANES), 0)
        value = jnp.where(row < BINS - 1, value, -jnp.inf)
        bests.append(jnp.max(value, axis=0, keepdims=True))
    best = bests[0]
    for q in range(quads):
        gain_ref[q:q + 1, :] = bests[q]
        best = jnp.maximum(best, bests[q])
    best = jnp.broadcast_to(best, (8, LANES))
    move = width
    folded = best
    for s in range(1, slots):
        folded = jnp.maximum(folded, pltpu.roll(best, s * move, 1))
    best_out[...] = folded

    def best_copy(step):
        return pltpu.make_async_remote_copy(
            src_ref=best_out, dst_ref=best_in.at[step],
            send_sem=best_send.at[step], recv_sem=best_recv.at[step],
            device_id=at(me_g, lax.rem(me_d + step, devs)), device_id_type=pl.DeviceIdType.MESH,
        )

    for step in range(1, devs):
        best_copy(step).start()
    for step in range(1, devs):
        best_copy(step).wait()
        folded = jnp.maximum(folded, best_in[step])
    best_ref[...] = folded


def kernel_body(groups, devs, bin_index, gradient, hessian, child_id, smaller_side):
    rows, features = bin_index.shape
    leaves = smaller_side.shape[0]
    own_features = features // devs
    own_leaves = leaves // groups
    width = 2 * own_leaves
    slots = LANES // width
    quads = own_features // slots
    chips = devs // 2
    planes = chips // 2
    vmem = pl.BlockSpec(memory_space=pltpu.VMEM)
    hbm = pl.BlockSpec(memory_space=pltpu.HBM)
    gain, best = pl.pallas_call(
        functools.partial(kernel, groups, devs, leaves),
        out_shape=(
            jax.ShapeDtypeStruct((quads, LANES), jnp.float32),
            jax.ShapeDtypeStruct((8, LANES), jnp.float32),
        ),
        in_specs=[hbm, hbm, hbm, hbm, pl.BlockSpec(memory_space=pltpu.SMEM)],
        out_specs=(vmem, vmem),
        scratch_shapes=[
            pltpu.VMEM((rows, features), jnp.int32),
            pltpu.VMEM((rows // LANES, LANES), jnp.bfloat16),
            pltpu.VMEM((rows // LANES, LANES), jnp.bfloat16),
            pltpu.VMEM((rows // LANES, LANES), jnp.int32),
            pltpu.VMEM((2, rows // LANES, LANES), jnp.float32),
            pltpu.SemaphoreType.DMA((rows // STEP_ROWS,)),
            pltpu.SemaphoreType.DMA((3,)),
            pltpu.VMEM((features, rows), jnp.float32),
            pltpu.VMEM((rows, groups * LANES), jnp.bfloat16),
            pltpu.VMEM((chips, groups, quads * BINS, LANES), jnp.float32),
            pltpu.VMEM((chips, groups, quads * BINS, LANES), jnp.float32),
            pltpu.VMEM((planes, groups, quads * BINS, LANES), jnp.float32),
            pltpu.VMEM((planes, groups, quads * BINS, LANES), jnp.float32),
            pltpu.VMEM((planes, groups, quads * BINS, LANES), jnp.float32),
            pltpu.VMEM((groups, planes, quads * BINS, LANES), jnp.float32),
            pltpu.VMEM((groups, quads * BINS, LANES), jnp.float32),
            pltpu.VMEM((8, LANES), jnp.float32),
            pltpu.VMEM((devs, 8, LANES), jnp.float32),
            pltpu.SemaphoreType.DMA((chips,)),
            pltpu.SemaphoreType.DMA((chips,)),
            pltpu.SemaphoreType.DMA((planes,)),
            pltpu.SemaphoreType.DMA((planes,)),
            pltpu.SemaphoreType.DMA((groups, planes)),
            pltpu.SemaphoreType.DMA((groups, planes)),
            pltpu.SemaphoreType.DMA((groups,)),
            pltpu.SemaphoreType.DMA((groups,)),
            pltpu.SemaphoreType.DMA((devs,)),
            pltpu.SemaphoreType.DMA((devs,)),
        ],
        compiler_params=pltpu.CompilerParams(
            collective_id=0, has_side_effects=True, vmem_limit_bytes=63 * 1024 * 1024
        ),
    )(
        bin_index, gradient.reshape(rows // LANES, LANES), hessian.reshape(rows // LANES, LANES),
        child_id.reshape(rows // LANES, LANES), smaller_side,
    )
    best_gain = gain.reshape(quads, slots, width)[:, :, :own_leaves]
    best_gain = best_gain.transpose(2, 0, 1).reshape(own_leaves, own_features)
    return (best_gain, best[0, :own_leaves])


def fits(groups, devs, leaves, features, rows):
    if devs % 4 or devs < 8 or features % devs or leaves % groups:
        return False
    width = 2 * (leaves // groups)
    if LANES % width:
        return False
    slots = LANES // width
    own = features // devs
    return own % slots == 0 and own % 8 == 0 and rows % KCHUNK == 0 and devs <= 16


def solution(mesh):
    in_specs = (
        P(("group", "dev"), None),
        P(("group", "dev")),
        P(("group", "dev")),
        P(("group", "dev")),
        P(),
    )
    out_specs = (P("group", "dev"), P("group"))
    groups, devs = mesh.shape["group"], mesh.shape["dev"]

    def body(bin_index, gradient, hessian, child_id, smaller_side):
        rows, features = bin_index.shape
        args = (bin_index, gradient, hessian, child_id, smaller_side)
        if fits(groups, devs, smaller_side.shape[0], features, rows):
            return kernel_body(groups, devs, *args)
        return plain_body(*args)

    return jax.shard_map(body, mesh=mesh, in_specs=in_specs, out_specs=out_specs, check_vma=False)
```
